32 devices in a mesh: dp: 2 (over y), expert: 8 (over z, x), tensor: 2 (over core).
Axes of the slice: x: 2, y: 2, z: 4, core: 2. Of those that a mesh axis runs over, the one named last changes fastest.
Arguments:
- block_input: bfloat16 [4096, 2048], P(('dp', 'expert', 'tensor')), may hold values from -6 to 6
- query_weight: bfloat16 [2048, 3072], P('dp', 'tensor'), may hold values from -0.125 to 0.125
- latent_weight: bfloat16 [2048, 576], P('dp'), may hold values from -0.125 to 0.125
- expand_weight: bfloat16 [512, 4096], P('dp', 'tensor'), may hold values from -0.25 to 0.25
- output_weight: bfloat16 [2048, 2048], P('tensor', 'dp'), may hold values from -0.75 to 0.75
- shared_gate: bfloat16 [2048, 2816], P('dp', 'tensor'), may hold values from -0.125 to 0.125
- shared_up: bfloat16 [2048, 2816], P('dp', 'tensor'), may hold values from -0.125 to 0.125
- shared_down: bfloat16 [2816, 2048], P('tensor', 'dp'), may hold values from -0.109375 to 0.109375
- expert_gate: bfloat16 [16, 2048, 1408], P(('expert', 'tensor'), 'dp'), may hold values from -0.125 to 0.125
- expert_up: bfloat16 [16, 2048, 1408], P(('expert', 'tensor'), 'dp'), may hold values from -0.125 to 0.125
- expert_down: bfloat16 [16, 1408, 2048], P(('expert', 'tensor'), None, 'dp'), may hold values from -0.15625 to 0.15625
- attn_gain: float32 [2048], replicated, may hold values from 0.5 to 1.5
- latent_gain: float32 [512], replicated, may hold values from 0.5 to 1.5
- ffn_gain: float32 [2048], replicated, may hold values from 0.5 to 1.5
- route_weights: float32 [4096, 6], P(('dp', 'expert', 'tensor')), may hold values from 0.05 to 0.3
- route_ids: int32 [4096, 6], P(('dp', 'expert', 'tensor')), may hold values from 0 to 15, all different within a row; in each aligned block of 128 rows (0 to 127, 128 to 255, ...) at most 64 rows name the same one
- out_grad: bfloat16 [4096, 2048], P(('dp', 'expert', 'tensor')), may hold values from -6 to 6
Outputs:
- block_output: bfloat16 [4096, 2048], P(('dp', 'expert', 'tensor'))
- input_grad: bfloat16 [4096, 2048], P(('dp', 'expert', 'tensor'))
- query_weight_grad: float32 [2048, 3072], P(('dp', 'expert'), 'tensor')
- latent_weight_grad: float32 [2048, 576], P(('dp', 'expert', 'tensor'))
- expand_weight_grad: float32 [512, 4096], P(('dp', 'expert'), 'tensor')
- output_weight_grad: float32 [2048, 2048], P('tensor', ('dp', 'expert'))
- shared_gate_grad: float32 [2048, 2816], P(('dp', 'expert'), 'tensor')
- shared_up_grad: float32 [2048, 2816], P(('dp', 'expert'), 'tensor')
- shared_down_grad: float32 [2816, 2048], P('tensor', ('dp', 'expert'))
- expert_gate_grad: float32 [16, 2048, 1408], P(('expert', 'tensor'), 'dp')
- expert_up_grad: float32 [16, 2048, 1408], P(('expert', 'tensor'), 'dp')
- expert_down_grad: float32 [16, 1408, 2048], P(('expert', 'tensor'), None, 'dp')
- attn_gain_grad: float32 [2048], P(('dp', 'expert', 'tensor'))
- latent_gain_grad: float32 [512], P(('dp', 'expert', 'tensor'))
- ffn_gain_grad: float32 [2048], P(('dp', 'expert', 'tensor'))
The draws below stay inside these ranges and needn't reach their ends.
Inputs may be any that keep to these rules, and one draw needn't show every extreme that they name: `route_ids`: each row names 6 different experts. Among the 128 rows of one device no expert is named by more than 64 rows, and that many is reached.
All inputs are finite; a program needn't handle non-finite values.
Results may differ from the reference program's by a relative error of at most 0.02.
Values may be sent and summed in bfloat16 or wider, within the bound.
A program may use at most 256 MiB of HBM per device.

```python
import math
import jax
import jax.numpy as jnp
import numpy as np
from jax import lax

D = 2048
HEADS = 16
NOPE = 128
ROPE = 64
LATENT = 512
VHEAD = 128
FFE = 1408
TOP = 6
TOK_DEV = 128
SFF = 2816
EXPERTS = 16
CAP = 64
SEQ = 256
TOKENS = 4096
N_DP = 2
N_EXPERT = 8
N_TENSOR = 2


def shard_levels(key, extent, shards, smallest, high):
    def one(position, parts):
        heights = jax.random.uniform(jax.random.fold_in(jax.random.fold_in(key, 6), position), (parts,), jnp.float32, smallest / len(shards), high / len(shards))
        return jnp.repeat(jnp.exp(heights), extent[position] // parts).reshape((-1,) + (1,) * (len(extent) - position - 1))

    loudness = one(*shards[0])
    for cut in shards[1:]:
        loudness = loudness * one(*cut)
    return loudness


def assign_block(stream_key, own, number, rows, count, top, limit, skew):
    sequence = jax.random.permutation(stream_key, count)
    packed, ordinary = shares(count, rows * top, limit, skew, True), shares(count, rows * top, limit, skew, False)
    places = jnp.arange(count)

    def named(lengths, turn):
        used = int((lengths > 0).sum())
        fixed = max(1, used // 4)
        passed = fixed + (places - fixed + turn * (used - fixed)) % max(1, count - fixed)
        return jnp.zeros((count,), jnp.int32).at[sequence[jnp.where(places < fixed, places, passed)]].set(jnp.asarray(lengths, jnp.int32))

    lengths = jnp.where(number % 4 == 0, named(packed, number // 4), named(ordinary, number - number // 4 - 1))
    mixed = jax.random.permutation(jax.random.fold_in(own, 3), count)
    giver, sink = mixed[0:count // 2 * 2:2], mixed[1:count // 2 * 2:2]
    room = jnp.minimum(lengths[giver] - 1, limit - lengths[sink]) // 2
    room = jnp.where((giver == sequence[0]) | (sink == sequence[0]) | (lengths[sink] == 0), 0, jnp.maximum(room, 0))
    passed = jax.random.randint(jax.random.fold_in(own, 4), (count // 2,), 0, 1 << 20) % (room + 1)
    lengths = lengths.at[giver].add(-passed).at[sink].add(passed)
    labels = jnp.searchsorted(jnp.cumsum(lengths), jnp.arange(rows * top), side="right").astype(jnp.int32)
    grid = labels.reshape(top, rows).T
    grid = grid[jax.random.permutation(jax.random.fold_in(own, 1), rows)]
    turn = jax.random.randint(jax.random.fold_in(own, 2), (rows, 1), 0, top)
    return jnp.take_along_axis(grid, (jnp.arange(top)[None, :] + turn) % top, axis=1)


def shares(count, total, limit, lean, full):
    loads = [(1 << 20) // math.isqrt(rank ** lean) + 1 for rank in range(1, count + 1)]
    largest = limit if full else min(limit, max(-(-total // count), total * loads[0] // sum(loads)))
    least = 1 if total - largest >= count - 1 else 0
    given, spare = [largest] + [least] * (count - 1), total - largest - least * (count - 1)
    while spare > 0:
        movable = [i for i in range(1, count) if given[i] < largest] or [i for i in range(1, count) if given[i] < limit]
        whole, left = sum([loads[i] for i in movable]), spare
        for i in movable:
            addition = min(limit - given[i], max(1, left * loads[i] // whole), spare)
            given[i] = given[i] + addition
            spare = spare - addition
    return np.array(given)


def centred(key, extent, spread, reach, shards=(), kind=jnp.bfloat16):
    drawn = spread * jax.random.normal(key, extent, jnp.float32)
    if shards:
        drawn = drawn * shard_levels(key, extent, shards, -0.22, 0.18)
    return jnp.clip(drawn, -reach, reach).astype(kind)


def setup_inputs(seed: int = 0) -> dict:
    keys = jax.random.split(jax.random.key(seed), 18)
    block_input = centred(keys[0], (TOKENS, D), 1.0, 6.0, ((0, 32),))
    query_weight = centred(keys[1], (D, HEADS * (NOPE + ROPE)), D ** -0.5, 0.125, ((0, 2), (1, 2)))
    latent_weight = centred(keys[2], (D, LATENT + ROPE), D ** -0.5, 0.125, ((0, 2),))
    expand_weight = centred(keys[3], (LATENT, HEADS * (NOPE + VHEAD)), LATENT ** -0.5, 0.25, ((0, 2), (1, 2)))
    output_weight = centred(keys[4], (HEADS * VHEAD, D), (HEADS * VHEAD // 32) ** -0.5, 0.75, ((0, 2), (1, 2)))
    shared_gate = centred(keys[5], (D, SFF), D ** -0.5, 0.125, ((0, 2), (1, 2)))
    shared_up = centred(keys[6], (D, SFF), D ** -0.5, 0.125, ((0, 2), (1, 2)))
    shared_down = centred(keys[7], (SFF, D), SFF ** -0.5, 0.109375, ((0, 2), (1, 2)))
    expert_gate = centred(keys[8], (EXPERTS, D, FFE), D ** -0.5, 0.125, ((0, 16), (1, 2)))
    expert_up = centred(keys[9], (EXPERTS, D, FFE), D ** -0.5, 0.125, ((0, 16), (1, 2)))
    expert_down = centred(keys[10], (EXPERTS, FFE, D), FFE ** -0.5, 0.15625, ((0, 16), (2, 2)))
    attn_gain = jnp.clip(1.0 + 0.1 * jax.random.normal(keys[11], (D,), jnp.float32), 0.5, 1.5)
    latent_gain = jnp.clip(1.0 + 0.1 * jax.random.normal(keys[12], (LATENT,), jnp.float32), 0.5, 1.5)
    ffn_gain = jnp.clip(1.0 + 0.1 * jax.random.normal(keys[13], (D,), jnp.float32), 0.5, 1.5)
    route_weights = jnp.clip(0.05 + 0.25 * jax.random.uniform(keys[14], (TOKENS, TOP), jnp.float32) ** shard_levels(keys[14], (TOKENS, TOP), ((0, 32),), -0.2, 0.2), 0.05, 0.3)
    route_ids_keys = jax.random.split(jax.random.fold_in(keys[15], 1), TOKENS // TOK_DEV)
    route_ids_turns = jax.random.permutation(jax.random.fold_in(keys[15], 3), TOKENS // TOK_DEV)
    route_ids = jax.vmap(lambda own, number: assign_block(jax.random.fold_in(keys[15], 2), own, number, TOK_DEV, EXPERTS, TOP, CAP, 2))(route_ids_keys, route_ids_turns).reshape((TOKENS, TOP))
    out_grad = centred(keys[16], (TOKENS, D), 1.0, 6.0, ((0, 32),))
    return dict(block_input=block_input, query_weight=query_weight, latent_weight=latent_weight, expand_weight=expand_weight, output_weight=output_weight, shared_gate=shared_gate, shared_up=shared_up, shared_down=shared_down, expert_gate=expert_gate, expert_up=expert_up, expert_down=expert_down, attn_gain=attn_gain, latent_gain=latent_gain, ffn_gain=ffn_gain, route_weights=route_weights, route_ids=route_ids, out_grad=out_grad)


EPSILON = 1e-06
HIGHEST = lax.Precision.HIGHEST

@jax.custom_vjp
def low(v):
    return lax.optimization_barrier(v.astype(jnp.bfloat16)).astype(jnp.float32)

@jax.custom_vjp
def low_back(v):
    return v

def low_keep(v):
    return (low(v), None)

def low_pass(kept, grad):
    return (grad,)

def back_keep(v):
    return (v, None)

def back_low(kept, grad):
    return (low(grad),)
low.defvjp(low_keep, low_pass)
low_back.defvjp(back_keep, back_low)

def matmul(first_operand, second_operand):
    return jnp.dot(first_operand, second_operand, precision=HIGHEST)

def rms_scale(values, gain_vector):
    return values * lax.rsqrt(lax.optimization_barrier(jnp.mean(values * values, axis=-1, keepdims=True)) + EPSILON) * gain_vector

def rope_tables(positions, rope_width):
    half_size = rope_width // 2
    frequency = 10000.0 ** (-jnp.arange(half_size).astype(jnp.float32) * (2.0 / rope_width))
    angles = positions[:, None] * frequency[None, :]
    return (jnp.cos(angles), jnp.sin(angles))

def rotate(vectors, cosine, sine_part):
    half_size = vectors.shape[-1] // 2
    first_half = vectors[..., :half_size]
    second_half = vectors[..., half_size:]
    return jnp.concatenate([first_half * cosine - second_half * sine_part, second_half * cosine + first_half * sine_part], axis=-1)

def attend_one(member, query_weight, expand_weight, output_weight):
    attn_in, latent, key_rope = member
    seq_len = attn_in.shape[0]
    cosine, sine_part = rope_tables(jnp.arange(seq_len).astype(jnp.float32), ROPE)
    query_raw = low_back(matmul(attn_in, query_weight)).reshape(seq_len, HEADS, NOPE + ROPE)
    query_rot = rotate(query_raw[:, :, NOPE:], cosine[:, None, :], sine_part[:, None, :])
    queries = low(jnp.concatenate([query_raw[:, :, :NOPE], query_rot], axis=-1))
    expanded = low(low_back(matmul(latent, expand_weight))).reshape(seq_len, HEADS, NOPE + VHEAD)
    scale_factor = 1.0 / math.sqrt(NOPE + ROPE)
    scores = jnp.einsum('qhc,khc->hqk', queries[:, :, :NOPE], expanded[:, :, :NOPE], precision=HIGHEST)
    scores = scores + jnp.einsum('qhc,kc->hqk', queries[:, :, NOPE:], key_rope, precision=HIGHEST)
    scores = low_back(scores * scale_factor)
    causal = jnp.arange(seq_len)[:, None] >= jnp.arange(seq_len)[None, :]
    exponent_terms = jnp.where(causal[None], jnp.exp(scores), 0.0)
    probabilities = exponent_terms / lax.optimization_barrier(jnp.sum(exponent_terms, axis=-1, keepdims=True))
    context = jnp.einsum('hqk,khc->qhc', low(probabilities), expanded[:, :, NOPE:], precision=HIGHEST)
    context = low(low_back(context.reshape(seq_len, HEADS * VHEAD)))
    return matmul(context, output_weight)

def reference(block_input, query_weight, latent_weight, expand_weight, output_weight, shared_gate, shared_up, shared_down, expert_gate, expert_up, expert_down, attn_gain, latent_gain, ffn_gain, route_weights, route_ids, out_grad):
    flat_routes = route_ids.reshape(-1).astype(jnp.int32)
    pair_total = flat_routes.shape[0]
    order_ids = jnp.argsort(flat_routes, stable=True).astype(jnp.int32)
    counts = lax.optimization_barrier(jnp.sum((flat_routes[:, None] == jnp.arange(EXPERTS, dtype=jnp.int32)[None, :]).astype(jnp.int32), axis=0))
    starts = (jnp.cumsum(counts) - counts).astype(jnp.int32)
    largest = N_DP * N_EXPERT * N_TENSOR * CAP
    slot_index = jnp.arange(largest, dtype=jnp.int32)
    pairing_table = order_ids[jnp.minimum(starts[:, None] + slot_index[None, :], pair_total - 1)]
    slot_is_valid = slot_index[None, :] < counts[:, None]
    gate_floats = route_weights.astype(jnp.float32)

    def block_forward(source_device, query_projection_weight, latent_down_weight, latent_expand_weight, attention_output_weight, common_gate_weight, common_up_weight, common_down_weight, routed_gate_weight, routed_up_weight, routed_down_weight, attention_norm_scale, latent_norm_scale, feedforward_norm_scale):
        attn_in = low(rms_scale(source_device, attention_norm_scale))
        compressed = low_back(matmul(attn_in, latent_down_weight))
        latent = low(rms_scale(compressed[:, :LATENT], latent_norm_scale))
        cosine, sine_part = rope_tables((jnp.arange(TOKENS, dtype=jnp.int32) % SEQ).astype(jnp.float32), ROPE)
        key_rope = low(rotate(compressed[:, LATENT:], cosine, sine_part))
        seq_count = TOKENS // SEQ
        per_step = math.gcd(seq_count, max(1, 4096 // SEQ))

        def attend_group(seq_group):
            return jax.vmap(lambda member: attend_one(member, query_projection_weight, latent_expand_weight, attention_output_weight))(seq_group)
        grouped = tuple((array_part.reshape(seq_count // per_step, per_step, SEQ, array_part.shape[-1]) for array_part in (attn_in, latent, key_rope)))
        attention = lax.map(jax.checkpoint(attend_group), grouped).reshape(TOKENS, D)
        hidden = source_device + low_back(attention)
        ffn_in = low(rms_scale(hidden, feedforward_norm_scale))
        shared_gate_pre = low_back(matmul(ffn_in, common_gate_weight))
        shared_up_pre = low_back(matmul(ffn_in, common_up_weight))
        shared_act = low(jax.nn.silu(shared_gate_pre) * shared_up_pre)
        shared_out = matmul(shared_act, common_down_weight)

        def single_expert(expert_item):
            pair_ids, valid_slots, weight_gate, up_weight_matrix, weight_down = expert_item
            expert_rows = low_back(ffn_in[pair_ids // TOP])
            gate_pre = low_back(matmul(expert_rows, weight_gate))
            up_pre = low_back(matmul(expert_rows, up_weight_matrix))
            expert_act = low(jax.nn.silu(gate_pre) * up_pre)
            expert_out = low(low_back(matmul(expert_act, weight_down)))
            return jnp.where(valid_slots[:, None], expert_out, 0.0)
        output_values = lax.map(jax.checkpoint(single_expert), (pairing_table, slot_is_valid, routed_gate_weight, routed_up_weight, routed_down_weight))
        pair_out = jnp.zeros((pair_total, D), jnp.float32).at[pairing_table.reshape(-1)].add(output_values.reshape(-1, D))
        routed = lax.optimization_barrier(jnp.sum(pair_out.reshape(TOKENS, TOP, D) * gate_floats[:, :, None], axis=1))
        return hidden + shared_out + routed
    floats = tuple((member.astype(jnp.float32) for member in (block_input, query_weight, latent_weight, expand_weight, output_weight, shared_gate, shared_up, shared_down, expert_gate, expert_up, expert_down, attn_gain, latent_gain, ffn_gain)))
    primal, pullback = jax.vjp(block_forward, *floats)
    gradients = pullback(out_grad.astype(jnp.float32))
    return (primal.astype(jnp.bfloat16), gradients[0].astype(jnp.bfloat16), gradients[1], gradients[2], gradients[3], gradients[4], gradients[5], gradients[6], gradients[7], gradients[8], gradients[9], gradients[10], gradients[11], gradients[12], gradients[13])
```

```python
import math

import jax
import jax.numpy as jnp
from jax import lax
from jax.sharding import PartitionSpec as P

D = 2048
NOPE = 128
ROPE = 64
LATENT = 512
VHEAD = 128
TOP = 6
BLOCK = 32
TOK_DEV = 128

EPSILON = 1e-06
F32 = jnp.float32
BF16 = jnp.bfloat16


def rms_forward(values, gain_vector):
    inverse = lax.rsqrt(jnp.mean(values * values, axis=-1, keepdims=True) + EPSILON)
    return (values * inverse * gain_vector, inverse)


def rms_backward(values, inverse, gain_vector, upstream):
    scaled = upstream * gain_vector
    inner_mean = jnp.mean(scaled * values, axis=-1, keepdims=True)
    return inverse * scaled - values * (inverse * inverse * inverse) * inner_mean


def rope_tables(positions, rope_width):
    half_size = rope_width // 2
    frequency = 10000.0 ** (-jnp.arange(half_size).astype(F32) * (2.0 / rope_width))
    angles = positions[:, None] * frequency[None, :]
    return (jnp.cos(angles), jnp.sin(angles))


def rotate(vectors, cosine, sine_part):
    half_size = vectors.shape[-1] // 2
    first_half = vectors[..., :half_size]
    second_half = vectors[..., half_size:]
    return jnp.concatenate(
        [
            first_half * cosine - second_half * sine_part,
            second_half * cosine + first_half * sine_part,
        ],
        axis=-1,
    )


def silu_parts(gate_pre):
    sigmoid_value = jax.nn.sigmoid(gate_pre)
    return (gate_pre * sigmoid_value, sigmoid_value * (1.0 + gate_pre * (1.0 - sigmoid_value)))


def matmul(a, b):
    return jnp.dot(a, b, preferred_element_type=F32)


def matmul_nt(a, b):
    return lax.dot_general(a, b, (((1,), (1,)), ((), ())), preferred_element_type=F32)


def matmul_tn(a, b):
    return lax.dot_general(a, b, (((0,), (0,)), ((), ())), preferred_element_type=F32)


def total(terms):
    result = terms[0]
    for term in terms[1:]:
        result = result + term
    return result


def ring_order(n_e):
    rows = 4 if n_e % 4 == 0 else 1
    cols = n_e // rows
    if rows == 1 or cols == 1:
        return list(range(n_e))
    order = [r * cols for r in range(rows)]
    for r in reversed(range(rows)):
        span = list(range(1, cols))
        if (rows - 1 - r) % 2 == 1:
            span.reverse()
        order += [r * cols + c for c in span]
    return order


def body(
    block_input,
    query_weight,
    latent_weight,
    expand_weight,
    output_weight,
    shared_gate,
    shared_up,
    shared_down,
    expert_gate,
    expert_up,
    expert_down,
    attn_gain,
    latent_gain,
    ffn_gain,
    route_weights,
    route_ids,
    out_grad,
):
    n_dp = lax.axis_size("dp")
    n_e = lax.axis_size("expert")
    n_t = lax.axis_size("tensor")
    dp = lax.axis_index("dp")
    ex = lax.axis_index("expert")
    tn = lax.axis_index("tensor")
    blk = D // n_dp
    lat_blk = LATENT // n_dp
    dps = range(n_dp)
    tok = block_input.shape[0]
    seq = tok * n_t

    def swap(x):
        return lax.ppermute(x, "tensor", [(0, 1), (1, 0)])

    def from_dp(x, j):
        return lax.ppermute(x, "dp", [((i + j) % n_dp, i) for i in dps])

    def to_dp(x, j):
        return lax.ppermute(x, "dp", [(i, (i + j) % n_dp) for i in dps])

    ring = ring_order(n_e)
    ring_pos = [ring.index(e) for e in range(n_e)]
    ring_perm = []
    for p in range(n_e):
        ring_perm.append((ring[p] * n_t, ring[(p + 1) % n_e] * n_t))
        ring_perm.append((ring[p] * n_t + 1, ring[(p - 1) % n_e] * n_t + 1))
    my_pos = jnp.array(ring_pos, jnp.int32)[ex]
    offsets = jnp.arange(n_e, dtype=jnp.int32) * jnp.where(tn == 0, -1, 1)
    owner = jnp.array(ring, jnp.int32)[(my_pos + offsets + n_e) % n_e]

    def ring_step(x):
        return lax.ppermute(x, ("expert", "tensor"), ring_perm)

    def ring_gather(x):
        pieces = [x]
        for _ in range(n_e - 1):
            pieces.append(ring_step(pieces[-1]))
        return pieces

    def ring_reduce(chunk):
        moving = chunk(1).astype(BF16)
        for s in range(2, n_e + 1):
            arrived = ring_step(moving).astype(F32) + chunk(s % n_e).astype(F32)
            moving = arrived.astype(BF16)
        return arrived

    def roll_columns(x, width):
        doubled = jnp.concatenate([x, x], axis=-1)
        start = (0,) * (x.ndim - 1) + (dp * width,)
        return lax.dynamic_slice(doubled, start, x.shape)

    def unroll_columns(x, width):
        doubled = jnp.concatenate([x, x], axis=-1)
        start = (0,) * (x.ndim - 1) + (((n_dp - dp) % n_dp) * width,)
        return lax.dynamic_slice(doubled, start, x.shape)

    def both_cores(own, other):
        return jnp.where(
            tn == 0, jnp.concatenate([own, other], 0), jnp.concatenate([other, own], 0)
        )

    def own_rows(x):
        return lax.dynamic_slice_in_dim(x, tn * tok, tok, 0)

    def cols(x, j, width=None):
        width = blk if width is None else width
        return x[..., j * width : (j + 1) * width]

    def chip_slice(weight, axis):
        size = weight.shape[axis] // n_e
        return lax.dynamic_slice_in_dim(weight, ex * size, size, axis)

    def plane_blocks(weight):
        blocks = [weight]
        rows = weight.shape[0] // n_e
        for j in range(1, n_dp):
            pieces = ring_gather(from_dp(chip_slice(weight, 0), j))
            full = jnp.zeros(weight.shape, weight.dtype)
            for s, piece in enumerate(pieces):
                full = lax.dynamic_update_slice(full, piece, (owner[s] * rows, 0))
            blocks.append(full)
        return blocks

    x_own = roll_columns(block_input, blk)
    g_own = roll_columns(out_grad, blk)
    attn_gain_r = roll_columns(attn_gain, blk)
    ffn_gain_r = roll_columns(ffn_gain, blk)
    x_seq = both_cores(x_own, swap(x_own))
    g_seq = both_cores(g_own, swap(g_own))

    latent_blocks = [latent_weight]
    half_rows = latent_weight.shape[0] // n_t
    latent_half = lax.dynamic_slice_in_dim(latent_weight, tn * half_rows, half_rows, 0)
    for j in range(1, n_dp):
        arrived = from_dp(latent_half, j)
        latent_blocks.append(both_cores(arrived, swap(arrived)))
    query_blocks = plane_blocks(query_weight)
    expand_blocks = plane_blocks(expand_weight)
    output_blocks = plane_blocks(output_weight)

    sgate_slice, sup_slice = chip_slice(shared_gate, 1), chip_slice(shared_up, 1)
    sdown_slice = chip_slice(shared_down, 0)
    gate_own, up_own, down_own = expert_gate[0], expert_up[0], expert_down[0]
    gate_blocks = [gate_own] + [from_dp(gate_own, j) for j in range(1, n_dp)]
    sgate_blocks = [sgate_slice] + [from_dp(sgate_slice, j) for j in range(1, n_dp)]
    sup_blocks = [sup_slice] + [from_dp(sup_slice, j) for j in range(1, n_dp)]
    sdown_blocks = [sdown_slice] + [from_dp(sdown_slice, j) for j in range(1, n_dp)]
    up_blocks = [up_own] + [from_dp(up_own, j) for j in range(1, n_dp)]
    down_blocks = [down_own] + [from_dp(down_own, j) for j in range(1, n_dp)]

    local_heads = query_weight.shape[1] // (NOPE + ROPE)
    scale_factor = 1.0 / math.sqrt(NOPE + ROPE)
    source = x_seq.astype(F32)
    normed_first, inverse_first = rms_forward(source, attn_gain_r)
    attn_in = normed_first.astype(BF16)
    compressed = total([matmul(cols(attn_in, j), latent_blocks[j]) for j in dps])
    latent_part = compressed[:, :LATENT]
    latent_normed, inverse_latent = rms_forward(latent_part, latent_gain)
    latent_low = roll_columns(latent_normed.astype(BF16), lat_blk)
    cosine, sine = rope_tables(jnp.arange(seq).astype(F32), ROPE)
    key_rope = rotate(compressed[:, LATENT:], cosine, sine).astype(BF16)
    query_raw = total([matmul(cols(attn_in, j), query_blocks[j]) for j in dps])
    query_raw = query_raw.reshape(seq, local_heads, NOPE + ROPE)
    query_rot = rotate(query_raw[:, :, NOPE:], cosine[:, None, :], sine[:, None, :])
    query_nope = query_raw[:, :, :NOPE].astype(BF16)
    query_rope = query_rot.astype(BF16)
    expanded = total([matmul(cols(latent_low, j, lat_blk), expand_blocks[j]) for j in dps])
    expanded = expanded.astype(BF16).reshape(seq, local_heads, NOPE + VHEAD)
    key_nope = expanded[:, :, :NOPE]
    value_part = expanded[:, :, NOPE:]
    causal = jnp.arange(seq)[:, None] >= jnp.arange(seq)[None, :]

    scores = jnp.einsum("qhc,khc->hqk", query_nope, key_nope, preferred_element_type=F32)
    scores = scores + jnp.einsum("qhc,kc->hqk", query_rope, key_rope, preferred_element_type=F32)
    exponent_terms = jnp.where(causal[None], jnp.exp(scores * scale_factor), 0.0)
    probabilities = exponent_terms / jnp.sum(exponent_terms, axis=-1, keepdims=True)
    probs_low = probabilities.astype(BF16)
    context = jnp.einsum("hqk,khc->qhc", probs_low, value_part, preferred_element_type=F32)
    context_low = context.reshape(seq, local_heads * VHEAD).astype(BF16)
    partial = jnp.concatenate(
        [matmul(context_low, output_blocks[j]).astype(BF16) for j in dps], axis=1
    )
    attention = partial.astype(F32) + swap(partial).astype(F32)
    hidden = source + attention
    normed_second, inverse_second = rms_forward(hidden, ffn_gain_r)
    ffn_in = normed_second.astype(BF16)

    def plane_tokens(own, j):
        mine = ring_gather(cols(own, j))
        theirs = [swap(piece) for piece in mine]
        return jnp.concatenate(mine + theirs, axis=0)

    info = jnp.concatenate([route_ids.astype(F32), route_weights], axis=1)
    info_mine = ring_gather(info)
    info_all = jnp.concatenate(info_mine, axis=0)
    info_all = jnp.concatenate([info_all, swap(info_all)], axis=0)

    g_own_late, _ = lax.optimization_barrier((g_own, query_blocks[-1]))
    g_tok = [plane_tokens(g_own_late, j) for j in dps]
    ffn_own = own_rows(ffn_in)
    x_tok = [plane_tokens(ffn_own, j) for j in dps]

    experts_total = n_e * n_t
    capacity = BLOCK * (
        (4 * TOK_DEV * TOP + 3 * experts_total * BLOCK - 1) // (3 * experts_total * BLOCK)
    )
    groups = experts_total
    slots = groups * capacity
    my_expert = (ex * n_t + tn).astype(F32)
    hits = (info_all[:, :TOP] == my_expert).astype(F32)
    chosen = jnp.sum(hits, axis=1).reshape(groups, tok)
    weight_of = jnp.sum(hits * info_all[:, TOP:], axis=1).reshape(groups, tok)
    upper = (jnp.arange(tok)[:, None] <= jnp.arange(tok)[None, :]).astype(BF16)
    rank = matmul(chosen.astype(BF16), upper)
    slot_number = jnp.where(chosen > 0.0, rank, 0.0).astype(jnp.int32)
    picks = slot_number[:, None, :] == (jnp.arange(capacity, dtype=jnp.int32) + 1)[None, :, None]
    pick = picks.astype(BF16)
    slot_weight = jnp.sum(jnp.where(picks, weight_of[:, None, :], 0.0), axis=2).reshape(slots, 1)

    def to_slots(tokens):
        grouped = tokens.reshape(groups, tok, tokens.shape[-1])
        return jnp.einsum("bsi,bid->bsd", pick, grouped, preferred_element_type=F32).reshape(
            slots, tokens.shape[-1]
        )

    def to_tokens(rows):
        grouped = rows.reshape(groups, capacity, rows.shape[-1])
        return jnp.einsum("bsi,bsd->bid", pick, grouped, preferred_element_type=F32).reshape(
            groups * tok, rows.shape[-1]
        )

    def plane_reduce(term):
        low = term.astype(BF16)
        half = low.shape[0] // 2
        merged = low[:half].astype(F32) + swap(low[half:]).astype(F32)
        return ring_reduce(lambda s: merged[s * tok : (s + 1) * tok])

    x_rows = [to_slots(x_tok[j]).astype(BF16) for j in dps]
    g_rows = [(slot_weight * to_slots(g_tok[j])).astype(BF16) for j in dps]

    sgate_pre = total([matmul(x_tok[j], sgate_blocks[j]) for j in dps])
    sup_pre = total([matmul(x_tok[j], sup_blocks[j]) for j in dps])
    shared_silu, shared_slope = silu_parts(sgate_pre)
    shared_act = (shared_silu * sup_pre).astype(BF16)
    sact_grad = total([matmul_nt(g_tok[j], sdown_blocks[j]) for j in dps])
    sgate_back = (sact_grad * sup_pre * shared_slope).astype(BF16)
    sup_back = (sact_grad * shared_silu).astype(BF16)

    gate_pre = total([matmul(x_rows[j], gate_blocks[j]) for j in dps])
    up_pre = total([matmul(x_rows[j], up_blocks[j]) for j in dps])
    expert_silu, expert_slope = silu_parts(gate_pre)
    expert_act = (expert_silu * up_pre).astype(BF16)
    act_grad = total([matmul_nt(g_rows[j], down_blocks[j]) for j in dps])
    gate_back = (act_grad * up_pre * expert_slope).astype(BF16)
    up_back = (act_grad * expert_silu).astype(BF16)

    def dp_sum(make):
        parts = [None] * n_dp
        arrived = [to_dp(make(j).astype(BF16), j).astype(F32) for j in range(1, n_dp)]
        return total([make(0)] + arrived)

    edown_grad = dp_sum(lambda j: matmul_tn(expert_act, g_rows[j]))

    in_grad_parts = []
    for j in dps:
        row_grad = (
            matmul_nt(gate_back, gate_blocks[j]) + matmul_nt(up_back, up_blocks[j])
        ).astype(BF16)
        term = (
            to_tokens(row_grad)
            + matmul_nt(sgate_back, sgate_blocks[j])
            + matmul_nt(sup_back, sup_blocks[j])
        )
        in_grad_parts.append(plane_reduce(term))
    ffn_in_grad_own = jnp.concatenate(in_grad_parts, axis=1)

    egate_grad = dp_sum(lambda j: matmul_tn(x_rows[j], gate_back))
    eup_grad = dp_sum(lambda j: matmul_tn(x_rows[j], up_back))

    out_parts = []
    for j in dps:
        out_rows = (slot_weight * matmul(expert_act, down_blocks[j])).astype(BF16)
        out_parts.append(plane_reduce(to_tokens(out_rows) + matmul(shared_act, sdown_blocks[j])))
    hidden_own = own_rows(hidden)
    block_output = unroll_columns(
        (hidden_own + jnp.concatenate(out_parts, axis=1)).astype(BF16), blk
    )

    def shared_local(j):
        return jnp.concatenate(
            [
                matmul_tn(x_tok[j], sgate_back),
                matmul_tn(x_tok[j], sup_back),
                matmul_tn(g_tok[j], shared_act),
            ],
            axis=1,
        )

    shared_sum = dp_sum(shared_local).astype(BF16)
    piece_rows = shared_sum.shape[0] // n_e
    slice_units = shared_act.shape[1]

    def rows_for(index):
        return lax.dynamic_slice_in_dim(shared_sum, index * piece_rows, piece_rows, 0)

    shared_all = jnp.zeros((n_e, piece_rows, 3 * slice_units), BF16)
    shared_all = lax.dynamic_update_slice(shared_all, rows_for(ex)[None], (ex, 0, 0))
    for k in range(1, n_e):
        piece = lax.ppermute(rows_for(ex ^ k), "expert", [(i, i ^ k) for i in range(n_e)])
        shared_all = lax.dynamic_update_slice(shared_all, piece[None], (ex ^ k, 0, 0))
    shared_all = shared_all.astype(F32)

    def columns_of(part):
        picked = shared_all[:, :, part * slice_units : (part + 1) * slice_units]
        return picked.transpose(1, 0, 2).reshape(piece_rows, n_e * slice_units)

    sgate_grad, sup_grad = columns_of(0), columns_of(1)
    sdown_grad = (
        shared_all[:, :, 2 * slice_units :].transpose(0, 2, 1).reshape(n_e * slice_units, piece_rows)
    )

    in_low = ffn_in_grad_own.astype(BF16)
    ffn_in_grad = both_cores(in_low, swap(in_low)).astype(F32)
    hidden_grad = g_seq.astype(F32) + rms_backward(hidden, inverse_second, ffn_gain_r, ffn_in_grad)
    hidden_low = hidden_grad.astype(BF16)
    ffn_gain_grad = jnp.sum(ffn_in_grad_own * hidden_own * own_rows(inverse_second), axis=0)

    context_grad = total([matmul_nt(cols(hidden_low, j), output_blocks[j]) for j in dps])
    context_grad = context_grad.astype(BF16).reshape(seq, local_heads, VHEAD)
    prob_grad = jnp.einsum("qhc,khc->hqk", context_grad, value_part, preferred_element_type=F32)
    value_grad = jnp.einsum("hqk,qhc->khc", probs_low, context_grad, preferred_element_type=F32)
    score_grad = (
        probabilities * (prob_grad - jnp.sum(prob_grad * probabilities, axis=-1, keepdims=True))
    ).astype(BF16)
    query_nope_grad = scale_factor * jnp.einsum(
        "hqk,khc->qhc", score_grad, key_nope, preferred_element_type=F32
    )
    query_rope_grad = scale_factor * jnp.einsum(
        "hqk,kc->qhc", score_grad, key_rope, preferred_element_type=F32
    )
    key_nope_grad = scale_factor * jnp.einsum(
        "hqk,qhc->khc", score_grad, query_nope, preferred_element_type=F32
    )
    key_rope_grad = scale_factor * jnp.einsum(
        "hqk,qhc->kc", score_grad, query_rope, preferred_element_type=F32
    )
    query_rope_back = rotate(query_rope_grad, cosine[:, None, :], -sine[:, None, :])
    query_raw_grad = (
        jnp.concatenate([query_nope_grad, query_rope_back], axis=-1)
        .reshape(seq, local_heads * (NOPE + ROPE))
        .astype(BF16)
    )
    expanded_grad = (
        jnp.concatenate([key_nope_grad, value_grad], axis=-1)
        .reshape(seq, local_heads * (NOPE + VHEAD))
        .astype(BF16)
    )
    latent_in = jnp.concatenate([matmul_nt(expanded_grad, expand_blocks[j]) for j in dps], axis=1)
    latent_in = unroll_columns(latent_in.astype(BF16), lat_blk)
    low_rank = jnp.concatenate([latent_in, key_rope_grad.astype(BF16)], axis=1)
    low_rank = low_rank.astype(F32) + swap(low_rank).astype(F32)
    latent_in_grad = low_rank[:, :LATENT]
    latent_back = rms_backward(latent_part, inverse_latent, latent_gain, latent_in_grad)
    key_rope_back = rotate(low_rank[:, LATENT:], cosine, -sine)
    compressed_grad = jnp.concatenate([latent_back, key_rope_back], axis=-1).astype(BF16)

    attn_partial = jnp.concatenate(
        [matmul_nt(query_raw_grad, query_blocks[j]).astype(BF16) for j in dps], axis=1
    )
    other_partial = lax.dynamic_slice_in_dim(attn_partial, (1 - tn) * tok, tok, 0)
    compressed_own = own_rows(compressed_grad)
    attn_in_grad = (
        own_rows(attn_partial).astype(F32)
        + swap(other_partial).astype(F32)
        + jnp.concatenate([matmul_nt(compressed_own, latent_blocks[j]) for j in dps], axis=1)
    )
    source_own, inverse_own = own_rows(source), own_rows(inverse_first)
    input_part = rms_backward(source_own, inverse_own, attn_gain_r, attn_in_grad)
    input_grad = unroll_columns((own_rows(hidden_grad) + input_part).astype(BF16), blk)
    attn_gain_grad = jnp.sum(attn_in_grad * source_own * inverse_own, axis=0)
    latent_gain_grad = jnp.sum(
        own_rows(latent_in_grad) * own_rows(latent_part) * own_rows(inverse_latent), axis=0
    )

    def chip_sum(local, axis, size, base=0):
        sums = []
        for j in dps:
            whole = local(j).astype(BF16)
            stride = whole.shape[axis] // n_e
            sums.append(
                ring_reduce(
                    lambda s: lax.dynamic_slice_in_dim(
                        whole, owner[s] * stride + base, size, axis
                    )
                )
            )
        return total([sums[0]] + [to_dp(sums[j].astype(BF16), j).astype(F32) for j in range(1, n_dp)])

    output_grad = chip_sum(
        lambda j: matmul_tn(context_low, cols(hidden_low, j)), 1, blk // n_e
    )
    query_grad = chip_sum(lambda j: matmul_tn(cols(attn_in, j), query_raw_grad), 0, blk // n_e)
    expand_grad = chip_sum(
        lambda j: matmul_tn(cols(latent_low, j, lat_blk), expanded_grad), 0, lat_blk // n_e
    )
    latent_rows = blk // (n_e * n_t)
    latent_grad = chip_sum(
        lambda j: matmul_tn(cols(attn_in, j), compressed_grad), 0, latent_rows, tn * latent_rows
    )

    gains = jnp.concatenate(
        [
            unroll_columns(attn_gain_grad, blk),
            unroll_columns(ffn_gain_grad, blk),
            latent_gain_grad,
        ]
    ).reshape(-1, 128)
    gains = gains + swap(gains)
    for axis, size in (("expert", n_e), ("dp", n_dp)):
        k = 1
        while k < size:
            gains = gains + lax.ppermute(gains, axis, [(i, i ^ k) for i in range(size)])
            k *= 2
    gains = gains.reshape(-1)
    device = (dp * n_e + ex) * n_t + tn
    devices = n_dp * n_e * n_t

    def gain_part(start, length):
        size = length // devices
        return lax.dynamic_slice_in_dim(gains, start + device * size, size, 0)

    return (
        block_output,
        input_grad,
        query_grad,
        latent_grad,
        expand_grad,
        output_grad,
        sgate_grad,
        sup_grad,
        sdown_grad,
        egate_grad[None],
        eup_grad[None],
        edown_grad[None],
        gain_part(0, D),
        gain_part(2 * D, LATENT),
        gain_part(D, D),
    )


def solution(mesh):
    everyone = ("dp", "expert", "tensor")
    in_specs = (
        P(everyone, None),
        P("dp", "tensor"),
        P("dp", None),
        P("dp", "tensor"),
        P("tensor", "dp"),
        P("dp", "tensor"),
        P("dp", "tensor"),
        P("tensor", "dp"),
        P(("expert", "tensor"), "dp", None),
        P(("expert", "tensor"), "dp", None),
        P(("expert", "tensor"), None, "dp"),
        P(),
        P(),
        P(),
        P(everyone, None),
        P(everyone, None),
        P(everyone, None),
    )
    out_specs = (
        P(everyone, None),
        P(everyone, None),
        P(("dp", "expert"), "tensor"),
        P(everyone, None),
        P(("dp", "expert"), "tensor"),
        P("tensor", ("dp", "expert")),
        P(("dp", "expert"), "tensor"),
        P(("dp", "expert"), "tensor"),
        P("tensor", ("dp", "expert")),
        P(("expert", "tensor"), "dp", None),
        P(("expert", "tensor"), "dp", None),
        P(("expert", "tensor"), None, "dp"),
        P(everyone),
        P(everyone),
        P(everyone),
    )
    return jax.shard_map(body, mesh=mesh, in_specs=in_specs, out_specs=out_specs, check_vma=False)
```

```python
import functools
import math

import jax
import jax.numpy as jnp
from jax import lax
from jax.experimental import pallas as pl
from jax.experimental.pallas import tpu as pltpu
from jax.sharding import PartitionSpec as P

D = 2048
NOPE = 128
ROPE = 64
LATENT = 512
VHEAD = 128
TOP = 6
BLOCK = 32
TOK_DEV = 128

EPSILON = 1e-06
F32 = jnp.float32
BF16 = jnp.bfloat16


def rms_forward(values, gain_vector):
    inverse = lax.rsqrt(jnp.mean(values * values, axis=-1, keepdims=True) + EPSILON)
    return (values * inverse * gain_vector, inverse)


def rms_backward(values, inverse, gain_vector, upstream):
    scaled = upstream * gain_vector
    inner_mean = jnp.mean(scaled * values, axis=-1, keepdims=True)
    return inverse * scaled - values * (inverse * inverse * inverse) * inner_mean


def rope_tables(positions, rope_width):
    half_size = rope_width // 2
    frequency = 10000.0 ** (-jnp.arange(half_size).astype(F32) * (2.0 / rope_width))
    angles = positions[:, None] * frequency[None, :]
    return (jnp.cos(angles), jnp.sin(angles))


def rotate(vectors, cosine, sine_part):
    half_size = vectors.shape[-1] // 2
    first_half = vectors[..., :half_size]
    second_half = vectors[..., half_size:]
    return jnp.concatenate(
        [
            first_half * cosine - second_half * sine_part,
            second_half * cosine + first_half * sine_part,
        ],
        axis=-1,
    )


def silu_parts(gate_pre):
    sigmoid_value = jax.nn.sigmoid(gate_pre)
    return (gate_pre * sigmoid_value, sigmoid_value * (1.0 + gate_pre * (1.0 - sigmoid_value)))


def matmul(a, b):
    return jnp.dot(a, b, preferred_element_type=F32)


def matmul_nt(a, b):
    return lax.dot_general(a, b, (((1,), (1,)), ((), ())), preferred_element_type=F32)


def matmul_tn(a, b):
    return lax.dot_general(a, b, (((0,), (0,)), ((), ())), preferred_element_type=F32)


def total(terms):
    result = terms[0]
    for term in terms[1:]:
        result = result + term
    return result


MESH = pl.DeviceIdType.MESH
ANY = pl.BlockSpec(memory_space=pl.ANY)
VMEM = pl.BlockSpec(memory_space=pltpu.VMEM)
DMA = pltpu.SemaphoreType.DMA
VMEM_BYTES = 60 * 1024 * 1024


RING_ROWS = 4


def chip_at(q, n_e):
    rows = RING_ROWS
    width = n_e // rows
    if width <= 1 or n_e % rows:
        return q
    back = q - rows
    i, k = back // (width - 1), back % (width - 1)
    col = jnp.where(i % 2 == 0, 1 + k, width - 1 - k)
    return jnp.where(q < rows, q * width, (rows - 1 - i) * width + col)


def place_of(e, n_e):
    rows = RING_ROWS
    width = n_e // rows
    if width <= 1 or n_e % rows:
        return e
    r, c = e // width, e % width
    i = rows - 1 - r
    k = jnp.where(i % 2 == 0, c - 1, width - 1 - c)
    return jnp.where(c == 0, r, rows + i * (width - 1) + k)


def chip_static(q, n_e):
    rows = RING_ROWS
    width = n_e // rows
    if width <= 1 or n_e % rows:
        return q
    if q < rows:
        return q * width
    i, k = (q - rows) // (width - 1), (q - rows) % (width - 1)
    return (rows - 1 - i) * width + (1 + k if i % 2 == 0 else width - 1 - k)


class Place:
    def __init__(self, sizes):
        self.n_dp, self.n_e, self.n_t = sizes
        self.dp = lax.axis_index("dp")
        self.ex = lax.axis_index("expert")
        self.tn = lax.axis_index("tensor")
        self.pos = place_of(self.ex, self.n_e)
        self.way = jnp.where(self.tn == 0, 1, -1)
        self.next = {"expert": self.owner(-1)}
        self.prev = {"expert": self.owner(1)}
        self.twin = {"tensor": 1 - self.tn}

    def owner(self, s):
        return chip_at((self.pos - self.way * s + 2 * self.n_e) % self.n_e, self.n_e)

    def group(self, j):
        return {"dp": (self.dp + j) % self.n_dp}

    def barrier(self, ring=True, twin=True, groups=True):
        peers = []
        if ring:
            peers += [self.next, self.prev]
        if twin:
            peers += [self.twin]
        if groups:
            peers += [self.group(j) for j in range(1, self.n_dp)]
        sem = pltpu.get_barrier_semaphore()
        for peer in peers:
            pl.semaphore_signal(sem, inc=1, device_id=peer, device_id_type=MESH)
        pl.semaphore_wait(sem, len(peers))


def remote(src, dst, send, recv, peer):
    return pltpu.make_async_remote_copy(
        src_ref=src, dst_ref=dst, send_sem=send, recv_sem=recv, device_id=peer, device_id_type=MESH
    )


def weights_kernel(sizes, n_ring, n_direct, *refs):
    n_in = n_ring + 1 + n_direct
    ins, outs = refs[:n_in], refs[n_in : 2 * n_in]
    y_send, y_recv, r_send, r_recv, t_send, t_recv = refs[2 * n_in :]
    here = Place(sizes)
    n_dp, n_e = here.n_dp, here.n_e
    here.barrier()

    def share(w, chip):
        rows = ins[w].shape[0] // n_e
        return pl.ds(pl.multiple_of(chip * rows, rows), rows)

    half = ins[n_ring].shape[0] // here.n_t
    half_rows = pl.ds(pl.multiple_of(here.tn * half, half), half)

    def fetch(w, j):
        if w < n_ring:
            src, dst = ins[w].at[share(w, here.ex)], outs[w].at[j - 1, share(w, here.ex)]
        elif w == n_ring:
            src, dst = ins[w].at[half_rows], outs[w].at[j - 1, half_rows]
        else:
            src, dst = ins[w], outs[w].at[j - 1]
        return remote(src, dst, y_send.at[w, j - 1], y_recv.at[w, j - 1], here.group(n_dp - j))

    def pass_on(w, j, s):
        piece = outs[w].at[j - 1, share(w, here.owner(s - 1))]
        return remote(
            piece, piece, r_send.at[w, j - 1, s - 1], r_recv.at[w, j - 1, s - 1], here.next
        )

    def arriving(w, j, s):
        piece = outs[w].at[j - 1, share(w, here.owner(s))]
        return remote(
            piece, piece, r_send.at[w, j - 1, s - 1], r_recv.at[w, j - 1, s - 1], here.next
        )

    def to_twin(j):
        piece = outs[n_ring].at[j - 1, half_rows]
        return remote(piece, piece, t_send.at[j - 1], t_recv.at[j - 1], here.twin)

    def from_twin(j):
        piece = outs[n_ring].at[j - 1, pl.ds(pl.multiple_of((1 - here.tn) * half, half), half)]
        return remote(piece, piece, t_send.at[j - 1], t_recv.at[j - 1], here.twin)

    order = [n_ring] + list(range(n_ring)) + list(range(n_ring + 1, n_in))
    groups = range(1, n_dp)
    for w in order:
        for j in groups:
            fetch(w, j).start()
    for j in groups:
        fetch(n_ring, j).wait_recv()
        to_twin(j).start()
    for s in range(1, n_e):
        for w in range(n_ring):
            for j in groups:
                if s == 1:
                    fetch(w, j).wait_recv()
                else:
                    arriving(w, j, s - 1).wait_recv()
                pass_on(w, j, s).start()
    for w in range(n_ring):
        for j in groups:
            arriving(w, j, n_e - 1).wait_recv()
    for j in groups:
        from_twin(j).wait_recv()
        to_twin(j).wait_send()
    for w in range(n_ring + 1, n_in):
        for j in groups:
            fetch(w, j).wait_recv()
    for w in range(n_in):
        for j in groups:
            fetch(w, j).wait_send()
    for s in range(1, n_e):
        for w in range(n_ring):
            for j in groups:
                pass_on(w, j, s).wait_send()


def gather_weights(sizes, ring, split, direct):
    ins = list(ring) + [split] + list(direct)
    n_dp, n_e, _ = sizes
    d = n_dp - 1
    return pl.pallas_call(
        functools.partial(weights_kernel, sizes, len(ring), len(direct)),
        out_shape=[jax.ShapeDtypeStruct((d,) + x.shape, x.dtype) for x in ins],
        in_specs=[ANY] * len(ins),
        out_specs=[ANY] * len(ins),
        scratch_shapes=[
            DMA((len(ins), d)),
            DMA((len(ins), d)),
            DMA((len(ring), d, n_e - 1)),
            DMA((len(ring), d, n_e - 1)),
            DMA((d,)),
            DMA((d,)),
        ],
        compiler_params=pltpu.CompilerParams(collective_id=0, has_side_effects=True),
        name="gather_weights",
    )(*ins)


def tokens_kernel(sizes, seq_ref, out_ref, r_send, r_recv, t_send, t_recv, l_sem):
    here = Place(sizes)
    n_e = here.n_e
    tok = seq_ref.shape[0] // here.n_t
    part = tok // 2
    here.barrier(groups=False)

    def own(core, h):
        return seq_ref.at[pl.ds(pl.multiple_of(core * tok + h * part, part), part)]

    def slot(s, h):
        return out_ref.at[pl.ds(s * tok + h * part, part)]

    def pass_on(s, h):
        src = own(here.tn, h) if s == 1 else slot(s - 1, h)
        return remote(src, slot(s, h), r_send.at[s - 1, h], r_recv.at[s - 1, h], here.next)

    def to_twin(s, h):
        return remote(
            slot(s, h), slot(n_e + s, h), t_send.at[s - 1, h], t_recv.at[s - 1, h], here.twin
        )

    local = []
    for h in range(2):
        pass_on(1, h).start()
    for h in range(2):
        local.append(pltpu.make_async_copy(own(here.tn, h), slot(0, h), l_sem.at[0, h]))
        local.append(pltpu.make_async_copy(own(1 - here.tn, h), slot(n_e, h), l_sem.at[1, h]))
    for copy in local:
        copy.start()
    for s in range(1, n_e):
        for h in range(2):
            pass_on(s, h).wait_recv()
            if s < n_e - 1:
                pass_on(s + 1, h).start()
            to_twin(s, h).start()
    for copy in local:
        copy.wait()
    for s in range(1, n_e):
        for h in range(2):
            to_twin(s, h).wait_recv()
            to_twin(s, h).wait_send()
            pass_on(s, h).wait_send()


def gather_tokens(sizes, seq_rows, collective_id):
    n_dp, n_e, n_t = sizes
    rows = seq_rows.shape[0] * n_e
    return pl.pallas_call(
        functools.partial(tokens_kernel, sizes),
        out_shape=jax.ShapeDtypeStruct((rows, seq_rows.shape[1]), seq_rows.dtype),
        in_specs=[VMEM],
        out_specs=ANY,
        scratch_shapes=[
            DMA((n_e - 1, 2)),
            DMA((n_e - 1, 2)),
            DMA((n_e - 1, 2)),
            DMA((n_e - 1, 2)),
            DMA((2, 2)),
        ],
        compiler_params=pltpu.CompilerParams(collective_id=collective_id, has_side_effects=True),
        name="gather_tokens",
    )(seq_rows)


def merge_kernel(sizes, flips, n_dp_blocks, *refs):
    n_pairs = len(flips)
    rows_ref, pick_ref = refs[:2]
    acts = refs[2 : 2 + n_pairs]
    first = 2 + n_pairs
    weights = [refs[first + p * n_dp_blocks : first + (p + 1) * n_dp_blocks] for p in range(n_pairs)]
    rest = refs[first + n_pairs * n_dp_blocks :]
    out_ref, away, back, mine, ring, t_send, t_recv, r_send, r_recv = rest
    here = Place(sizes)
    n_e = here.n_e
    groups, tok, cap = pick_ref.shape
    width = rows_ref.shape[1]
    blk = width // n_dp_blocks
    halves = 2
    part = width // halves
    here.barrier(groups=False)

    def term(group, put):
        pick = pick_ref[group]
        slots = pl.ds(pl.multiple_of(group * cap, cap), cap)
        tokens = pl.ds(pl.multiple_of(group * tok, tok), tok)
        for j in range(n_dp_blocks):
            columns = slice(j * blk, (j + 1) * blk)
            value = jnp.dot(pick, rows_ref[slots, columns], preferred_element_type=F32)
            for flip, act, blocks in zip(flips, acts, weights):
                if flip:
                    value += matmul_nt(act[tokens, :], blocks[j][...])
                else:
                    value += jnp.dot(act[tokens, :], blocks[j][...], preferred_element_type=F32)
            put(columns, value.astype(BF16))

    def store(ref, index):
        def put(columns, value):
            ref[index, :, columns] = value

        return put

    def to_twin(s):
        return remote(away.at[s], back.at[s], t_send.at[s], t_recv.at[s], here.twin)

    def pass_on(s, h):
        columns = pl.ds(h * part, part)
        return remote(
            ring.at[s - 1, :, columns],
            ring.at[s, :, columns],
            r_send.at[s - 1, h],
            r_recv.at[s - 1, h],
            here.next,
        )

    def prepare(s):
        term(n_e + s, store(away, s))
        to_twin(s).start()
        term(s, store(mine, s))

    prepare(1)
    prepare(2)
    to_twin(1).wait_recv()
    for h in range(halves):
        columns = slice(h * part, (h + 1) * part)
        merged = mine[1, :, columns].astype(F32) + back[1, :, columns].astype(F32)
        ring[0, :, columns] = merged.astype(BF16)
        pass_on(1, h).start()

    def step(s, carry):
        ahead = (s + 1) % n_e

        prepare(ahead)
        to_twin(s).wait_recv()
        for h in range(halves):
            columns = slice(h * part, (h + 1) * part)
            merged = mine[s, :, columns].astype(F32) + back[s, :, columns].astype(F32)
            pass_on(s - 1, h).wait_recv()
            merged += ring[s - 1, :, columns].astype(F32)
            ring[s - 1, :, columns] = merged.astype(BF16)
            pass_on(s, h).start()
        return carry

    lax.fori_loop(2, n_e, step, 0)
    to_twin(0).wait_recv()
    for h in range(halves):
        columns = slice(h * part, (h + 1) * part)
        merged = mine[0, :, columns].astype(F32) + back[0, :, columns].astype(F32)
        pass_on(n_e - 1, h).wait_recv()
        out_ref[:, columns] = merged + ring[n_e - 1, :, columns].astype(F32)
    for s in range(n_e):
        to_twin(s).wait_send()
    for s in range(1, n_e):
        for h in range(halves):
            pass_on(s, h).wait_send()


def merge_tokens(sizes, rows, pick, pairs, collective_id):
    n_dp, n_e, n_t = sizes
    tok, width = pick.shape[1], rows.shape[1]
    acts = [act for act, _, _ in pairs]
    blocks = [w for _, ws, _ in pairs for w in ws]
    flips = tuple(flip for _, _, flip in pairs)
    ins = [rows, pick] + acts + blocks
    held = pltpu.VMEM((n_e, tok, width), BF16)
    return pl.pallas_call(
        functools.partial(merge_kernel, sizes, flips, n_dp),
        out_shape=jax.ShapeDtypeStruct((tok, width), F32),
        in_specs=[VMEM] * len(ins),
        out_specs=VMEM,
        scratch_shapes=[
            held,
            held,
            held,
            held,
            DMA((n_e,)),
            DMA((n_e,)),
            DMA((n_e - 1, 2)),
            DMA((n_e - 1, 2)),
        ],
        compiler_params=pltpu.CompilerParams(
            collective_id=collective_id, has_side_effects=True, vmem_limit_bytes=VMEM_BYTES
        ),
        name="merge_tokens",
    )(*ins)


def sum_kernel(sizes, per_core, *refs):
    n = len(per_core)
    locals_, outs, bufs = refs[:n], refs[n : 2 * n], refs[2 * n : 3 * n]
    sent, came = refs[3 * n : 4 * n], refs[4 * n : 5 * n]
    r_send, r_recv, y_send, y_recv = refs[5 * n :]
    here = Place(sizes)
    n_dp, n_e = here.n_dp, here.n_e
    here.barrier(twin=False)

    def own(m, j, s):
        rows = outs[m].shape[0]
        start = here.owner(s) * rows
        if per_core[m]:
            start = start * here.n_t + here.tn * rows
        return locals_[m][j, pl.ds(pl.multiple_of(start, rows), rows), :].astype(F32)

    def pass_on(m, j, s):
        return remote(
            bufs[m].at[j, s - 1],
            bufs[m].at[j, s],
            r_send.at[m, j, s - 1],
            r_recv.at[m, j, s - 1],
            here.next,
        )

    def to_group(m, j):
        return remote(
            sent[m].at[j - 1],
            came[m].at[j - 1],
            y_send.at[m, j - 1],
            y_recv.at[m, j - 1],
            here.group(j),
        )

    far_first = [j for j in range(1, n_dp)] + [0]
    for m in range(n):
        for j in far_first:
            bufs[m][j, 0] = own(m, j, 1).astype(bufs[m].dtype)
            pass_on(m, j, 1).start()

    def step(s, carry):
        for m in range(n):
            for j in far_first:
                mine = own(m, j, s)
                pass_on(m, j, s - 1).wait_recv()
                moving = mine + bufs[m][j, s - 1].astype(F32)
                bufs[m][j, s - 1] = moving.astype(bufs[m].dtype)
                pass_on(m, j, s).start()
        return carry

    lax.fori_loop(2, n_e, step, 0)
    for m in range(n):
        for j in far_first:
            mine = own(m, j, 0)
            pass_on(m, j, n_e - 1).wait_recv()
            whole = mine + bufs[m][j, n_e - 1].astype(F32)
            if j == 0:
                outs[m][...] = whole
            else:
                sent[m][j - 1] = whole.astype(sent[m].dtype)
                to_group(m, j).start()
    for m in range(n):
        for j in range(1, n_dp):
            to_group(m, j).wait_recv()
            outs[m][...] += came[m][j - 1].astype(F32)
    for m in range(n):
        for j in range(1, n_dp):
            to_group(m, j).wait_send()
        for j in range(n_dp):
            for s in range(1, n_e):
                pass_on(m, j, s).wait_send()


def sum_chips(sizes, mats, per_core, collective_id):
    n_dp, n_e, n_t = sizes
    n = len(mats)
    shapes = []
    for mat, split in zip(mats, per_core):
        rows = mat.shape[1] // n_e // (n_t if split else 1)
        shapes.append((rows, mat.shape[2]))
    bufs = [pltpu.VMEM((n_dp, n_e) + s, mat.dtype) for s, mat in zip(shapes, mats)]
    hops = [pltpu.VMEM((n_dp - 1,) + s, mat.dtype) for s, mat in zip(shapes, mats)]
    return pl.pallas_call(
        functools.partial(sum_kernel, sizes, tuple(per_core)),
        out_shape=[jax.ShapeDtypeStruct(s, F32) for s in shapes],
        in_specs=[VMEM] * n,
        out_specs=[VMEM] * n,
        scratch_shapes=bufs
        + hops
        + hops
        + [
            DMA((n, n_dp, n_e - 1)),
            DMA((n, n_dp, n_e - 1)),
            DMA((n, n_dp - 1)),
            DMA((n, n_dp - 1)),
        ],
        compiler_params=pltpu.CompilerParams(
            collective_id=collective_id, has_side_effects=True, vmem_limit_bytes=VMEM_BYTES
        ),
        name="sum_chips",
    )(*mats)


def body(
    block_input,
    query_weight,
    latent_weight,
    expand_weight,
    output_weight,
    shared_gate,
    shared_up,
    shared_down,
    expert_gate,
    expert_up,
    expert_down,
    attn_gain,
    latent_gain,
    ffn_gain,
    route_weights,
    route_ids,
    out_grad,
):
    n_dp = lax.axis_size("dp")
    n_e = lax.axis_size("expert")
    n_t = lax.axis_size("tensor")
    dp = lax.axis_index("dp")
    ex = lax.axis_index("expert")
    tn = lax.axis_index("tensor")
    sizes = (n_dp, n_e, n_t)
    blk = D // n_dp
    lat_blk = LATENT // n_dp
    dps = range(n_dp)
    tok = block_input.shape[0]
    seq = tok * n_t

    def swap(x):
        return lax.ppermute(x, "tensor", [(0, 1), (1, 0)])

    def from_dp(x, j):
        return lax.ppermute(x, "dp", [((i + j) % n_dp, i) for i in dps])

    def to_dp(x, j):
        return lax.ppermute(x, "dp", [(i, (i + j) % n_dp) for i in dps])

    ring = [int(chip_static(p, n_e)) for p in range(n_e)]
    ring_perm = []
    for p in range(n_e):
        ring_perm.append((ring[p] * n_t, ring[(p + 1) % n_e] * n_t))
        ring_perm.append((ring[p] * n_t + 1, ring[(p - 1) % n_e] * n_t + 1))

    def ring_step(x):
        return lax.ppermute(x, ("expert", "tensor"), ring_perm)

    def ring_gather(x):
        pieces = [x]
        for _ in range(n_e - 1):
            pieces.append(ring_step(pieces[-1]))
        return pieces

    def roll_columns(x, width):
        doubled = jnp.concatenate([x, x], axis=-1)
        start = (0,) * (x.ndim - 1) + (dp * width,)
        return lax.dynamic_slice(doubled, start, x.shape)

    def unroll_columns(x, width):
        doubled = jnp.concatenate([x, x], axis=-1)
        start = (0,) * (x.ndim - 1) + (((n_dp - dp) % n_dp) * width,)
        return lax.dynamic_slice(doubled, start, x.shape)

    def both_cores(own, other):
        return jnp.where(
            tn == 0, jnp.concatenate([own, other], 0), jnp.concatenate([other, own], 0)
        )

    def own_rows(x):
        return lax.dynamic_slice_in_dim(x, tn * tok, tok, 0)

    def cols(x, j, width=None):
        width = blk if width is None else width
        return x[..., j * width : (j + 1) * width]

    def chip_slice(weight, axis):
        size = weight.shape[axis] // n_e
        return lax.dynamic_slice_in_dim(weight, ex * size, size, axis)

    x_own = roll_columns(block_input, blk)
    g_own = roll_columns(out_grad, blk)
    attn_gain_r = roll_columns(attn_gain, blk)
    ffn_gain_r = roll_columns(ffn_gain, blk)
    x_seq = both_cores(x_own, swap(x_own))
    g_seq = both_cores(g_own, swap(g_own))

    sgate_slice, sup_slice = chip_slice(shared_gate, 1), chip_slice(shared_up, 1)
    sdown_slice = chip_slice(shared_down, 0)
    gate_own, up_own, down_own = expert_gate[0], expert_up[0], expert_down[0]
    top = gate_own.shape[0] // 2
    fetched = gather_weights(
        sizes,
        [query_weight, output_weight, expand_weight],
        latent_weight,
        [sgate_slice, sup_slice, sdown_slice, gate_own[:top]],
    )
    groups_of = [[own] + [got[j] for j in range(n_dp - 1)] for own, got in zip(
        [query_weight, output_weight, expand_weight, latent_weight, sgate_slice, sup_slice, sdown_slice],
        fetched,
    )]
    query_blocks, output_blocks, expand_blocks, latent_blocks = groups_of[:4]
    sgate_blocks, sup_blocks, sdown_blocks = groups_of[4:]
    gate_rest, up_late, down_late, g_late, _ = lax.optimization_barrier(
        (gate_own[top:], up_own, down_own, g_own, fetched[-1])
    )
    gate_blocks = [gate_own] + [
        jnp.concatenate([fetched[-1][j - 1], from_dp(gate_rest, j)], axis=0)
        for j in range(1, n_dp)
    ]
    up_blocks = [up_own] + [from_dp(up_late, j) for j in range(1, n_dp)]
    down_blocks = [down_own] + [from_dp(down_late, j) for j in range(1, n_dp)]

    local_heads = query_weight.shape[1] // (NOPE + ROPE)
    scale_factor = 1.0 / math.sqrt(NOPE + ROPE)
    source = x_seq.astype(F32)
    normed_first, inverse_first = rms_forward(source, attn_gain_r)
    attn_in = normed_first.astype(BF16)
    compressed = total([matmul(cols(attn_in, j), latent_blocks[j]) for j in dps])
    latent_part = compressed[:, :LATENT]
    latent_normed, inverse_latent = rms_forward(latent_part, latent_gain)
    latent_low = roll_columns(latent_normed.astype(BF16), lat_blk)
    cosine, sine = rope_tables(jnp.arange(seq).astype(F32), ROPE)
    key_rope = rotate(compressed[:, LATENT:], cosine, sine).astype(BF16)
    query_raw = total([matmul(cols(attn_in, j), query_blocks[j]) for j in dps])
    query_raw = query_raw.reshape(seq, local_heads, NOPE + ROPE)
    query_rot = rotate(query_raw[:, :, NOPE:], cosine[:, None, :], sine[:, None, :])
    query_nope = query_raw[:, :, :NOPE].astype(BF16)
    query_rope = query_rot.astype(BF16)
    expanded = total([matmul(cols(latent_low, j, lat_blk), expand_blocks[j]) for j in dps])
    expanded = expanded.astype(BF16).reshape(seq, local_heads, NOPE + VHEAD)
    key_nope = expanded[:, :, :NOPE]
    value_part = expanded[:, :, NOPE:]
    causal = jnp.arange(seq)[:, None] >= jnp.arange(seq)[None, :]

    scores = jnp.einsum("qhc,khc->hqk", query_nope, key_nope, preferred_element_type=F32)
    scores = scores + jnp.einsum("qhc,kc->hqk", query_rope, key_rope, preferred_element_type=F32)
    exponent_terms = jnp.where(causal[None], jnp.exp(scores * scale_factor), 0.0)
    probabilities = exponent_terms / jnp.sum(exponent_terms, axis=-1, keepdims=True)
    probs_low = probabilities.astype(BF16)
    context = jnp.einsum("hqk,khc->qhc", probs_low, value_part, preferred_element_type=F32)
    context_low = context.reshape(seq, local_heads * VHEAD).astype(BF16)
    partial = jnp.concatenate(
        [matmul(context_low, output_blocks[j]).astype(BF16) for j in dps], axis=1
    )
    attention = partial.astype(F32) + swap(partial).astype(F32)
    hidden = source + attention
    normed_second, inverse_second = rms_forward(hidden, ffn_gain_r)
    ffn_in = normed_second.astype(BF16)

    def plane_rows(own):
        mine = jnp.concatenate(ring_gather(own), axis=0)
        return jnp.concatenate([mine, swap(mine)], axis=0)

    info_all = plane_rows(jnp.concatenate([route_ids.astype(F32), route_weights], axis=1))
    g_all = plane_rows(g_late)
    x_all = gather_tokens(sizes, ffn_in, 1)
    g_tok = [cols(g_all, j) for j in dps]
    x_tok = [cols(x_all, j) for j in dps]

    experts_total = n_e * n_t
    capacity = BLOCK * (
        (4 * TOK_DEV * TOP + 3 * experts_total * BLOCK - 1) // (3 * experts_total * BLOCK)
    )
    groups = experts_total
    slots = groups * capacity
    my_expert = (ex * n_t + tn).astype(F32)
    hits = (info_all[:, :TOP] == my_expert).astype(F32)
    chosen = jnp.sum(hits, axis=1).reshape(groups, tok)
    weight_of = jnp.sum(hits * info_all[:, TOP:], axis=1).reshape(groups, tok)
    upper = (jnp.arange(tok)[:, None] <= jnp.arange(tok)[None, :]).astype(BF16)
    rank = matmul(chosen.astype(BF16), upper)
    slot_number = jnp.where(chosen > 0.0, rank, 0.0).astype(jnp.int32)
    picks = slot_number[:, None, :] == (jnp.arange(capacity, dtype=jnp.int32) + 1)[None, :, None]
    pick = picks.astype(BF16)
    pick_t = pick.transpose(0, 2, 1)
    slot_weight = jnp.sum(jnp.where(picks, weight_of[:, None, :], 0.0), axis=2).reshape(slots, 1)

    def to_slots(tokens):
        grouped = tokens.reshape(groups, tok, tokens.shape[-1])
        return jnp.einsum("bsi,bid->bsd", pick, grouped, preferred_element_type=F32).reshape(
            slots, tokens.shape[-1]
        )

    x_rows = [to_slots(x_tok[j]).astype(BF16) for j in dps]
    g_rows = [(slot_weight * to_slots(g_tok[j])).astype(BF16) for j in dps]

    sgate_pre = total([matmul(x_tok[j], sgate_blocks[j]) for j in dps])
    sup_pre = total([matmul(x_tok[j], sup_blocks[j]) for j in dps])
    shared_silu, shared_slope = silu_parts(sgate_pre)
    shared_act = (shared_silu * sup_pre).astype(BF16)
    sact_grad = total([matmul_nt(g_tok[j], sdown_blocks[j]) for j in dps])
    sgate_back = (sact_grad * sup_pre * shared_slope).astype(BF16)
    sup_back = (sact_grad * shared_silu).astype(BF16)

    gate_pre = total([matmul(x_rows[j], gate_blocks[j]) for j in dps])
    up_pre = total([matmul(x_rows[j], up_blocks[j]) for j in dps])
    expert_silu, expert_slope = silu_parts(gate_pre)
    expert_act = (expert_silu * up_pre).astype(BF16)
    act_grad = total([matmul_nt(g_rows[j], down_blocks[j]) for j in dps])
    gate_back = (act_grad * up_pre * expert_slope).astype(BF16)
    up_back = (act_grad * expert_silu).astype(BF16)

    def dp_sum(make):
        parts = [None] * n_dp
        arrived = [to_dp(make(j).astype(BF16), j).astype(F32) for j in range(1, n_dp)]
        return total([make(0)] + arrived)

    edown_grad = dp_sum(lambda j: matmul_tn(expert_act, g_rows[j]))

    row_grad = jnp.concatenate(
        [
            (matmul_nt(gate_back, gate_blocks[j]) + matmul_nt(up_back, up_blocks[j])).astype(BF16)
            for j in dps
        ],
        axis=1,
    )
    ffn_in_grad_own = merge_tokens(
        sizes,
        row_grad,
        pick_t,
        [(sgate_back, sgate_blocks, True), (sup_back, sup_blocks, True)],
        2,
    )

    egate_grad = dp_sum(lambda j: matmul_tn(x_rows[j], gate_back))
    eup_grad = dp_sum(lambda j: matmul_tn(x_rows[j], up_back))

    out_rows = jnp.concatenate(
        [(slot_weight * matmul(expert_act, down_blocks[j])).astype(BF16) for j in dps], axis=1
    )
    ffn_out = merge_tokens(sizes, out_rows, pick_t, [(shared_act, sdown_blocks, False)], 3)
    hidden_own = own_rows(hidden)
    block_output = unroll_columns((hidden_own + ffn_out).astype(BF16), blk)

    def shared_local(j):
        return jnp.concatenate(
            [
                matmul_tn(x_tok[j], sgate_back),
                matmul_tn(x_tok[j], sup_back),
                matmul_tn(g_tok[j], shared_act),
            ],
            axis=1,
        )

    shared_sum = dp_sum(shared_local).astype(BF16)
    piece_rows = shared_sum.shape[0] // n_e
    slice_units = shared_act.shape[1]

    def rows_for(index):
        return lax.dynamic_slice_in_dim(shared_sum, index * piece_rows, piece_rows, 0)

    shared_all = jnp.zeros((n_e, piece_rows, 3 * slice_units), BF16)
    shared_all = lax.dynamic_update_slice(shared_all, rows_for(ex)[None], (ex, 0, 0))
    for k in range(1, n_e):
        piece = lax.ppermute(rows_for(ex ^ k), "expert", [(i, i ^ k) for i in range(n_e)])
        shared_all = lax.dynamic_update_slice(shared_all, piece[None], (ex ^ k, 0, 0))
    shared_all = shared_all.astype(F32)

    def columns_of(part):
        picked = shared_all[:, :, part * slice_units : (part + 1) * slice_units]
        return picked.transpose(1, 0, 2).reshape(piece_rows, n_e * slice_units)

    sgate_grad, sup_grad = columns_of(0), columns_of(1)
    sdown_grad = (
        shared_all[:, :, 2 * slice_units :].transpose(0, 2, 1).reshape(n_e * slice_units, piece_rows)
    )

    in_low = ffn_in_grad_own.astype(BF16)
    ffn_in_grad = both_cores(in_low, swap(in_low)).astype(F32)
    hidden_grad = g_seq.astype(F32) + rms_backward(hidden, inverse_second, ffn_gain_r, ffn_in_grad)
    hidden_low = hidden_grad.astype(BF16)
    ffn_gain_grad = jnp.sum(ffn_in_grad_own * hidden_own * own_rows(inverse_second), axis=0)

    context_grad = total([matmul_nt(cols(hidden_low, j), output_blocks[j]) for j in dps])
    context_grad = context_grad.astype(BF16).reshape(seq, local_heads, VHEAD)
    prob_grad = jnp.einsum("qhc,khc->hqk", context_grad, value_part, preferred_element_type=F32)
    value_grad = jnp.einsum("hqk,qhc->khc", probs_low, context_grad, preferred_element_type=F32)
    score_grad = (
        probabilities * (prob_grad - jnp.sum(prob_grad * probabilities, axis=-1, keepdims=True))
    ).astype(BF16)
    query_nope_grad = scale_factor * jnp.einsum(
        "hqk,khc->qhc", score_grad, key_nope, preferred_element_type=F32
    )
    query_rope_grad = scale_factor * jnp.einsum(
        "hqk,kc->qhc", score_grad, key_rope, preferred_element_type=F32
    )
    key_nope_grad = scale_factor * jnp.einsum(
        "hqk,qhc->khc", score_grad, query_nope, preferred_element_type=F32
    )
    key_rope_grad = scale_factor * jnp.einsum(
        "hqk,qhc->kc", score_grad, query_rope, preferred_element_type=F32
    )
    query_rope_back = rotate(query_rope_grad, cosine[:, None, :], -sine[:, None, :])
    query_raw_grad = (
        jnp.concatenate([query_nope_grad, query_rope_back], axis=-1)
        .reshape(seq, local_heads * (NOPE + ROPE))
        .astype(BF16)
    )
    expanded_grad = (
        jnp.concatenate([key_nope_grad, value_grad], axis=-1)
        .reshape(seq, local_heads * (NOPE + VHEAD))
        .astype(BF16)
    )
    latent_in = jnp.concatenate([matmul_nt(expanded_grad, expand_blocks[j]) for j in dps], axis=1)
    latent_in = unroll_columns(latent_in.astype(BF16), lat_blk)
    low_rank = jnp.concatenate([latent_in, key_rope_grad.astype(BF16)], axis=1)
    low_rank = low_rank.astype(F32) + swap(low_rank).astype(F32)
    latent_in_grad = low_rank[:, :LATENT]
    latent_back = rms_backward(latent_part, inverse_latent, latent_gain, latent_in_grad)
    key_rope_back = rotate(low_rank[:, LATENT:], cosine, -sine)
    compressed_grad = jnp.concatenate([latent_back, key_rope_back], axis=-1).astype(BF16)

    attn_partial = jnp.concatenate(
        [matmul_nt(query_raw_grad, query_blocks[j]).astype(BF16) for j in dps], axis=1
    )
    other_partial = lax.dynamic_slice_in_dim(attn_partial, (1 - tn) * tok, tok, 0)
    compressed_own = own_rows(compressed_grad)
    attn_in_grad = (
        own_rows(attn_partial).astype(F32)
        + swap(other_partial).astype(F32)
        + jnp.concatenate([matmul_nt(compressed_own, latent_blocks[j]) for j in dps], axis=1)
    )
    source_own, inverse_own = own_rows(source), own_rows(inverse_first)
    input_part = rms_backward(source_own, inverse_own, attn_gain_r, attn_in_grad)
    input_grad = unroll_columns((own_rows(hidden_grad) + input_part).astype(BF16), blk)
    attn_gain_grad = jnp.sum(attn_in_grad * source_own * inverse_own, axis=0)
    latent_gain_grad = jnp.sum(
        own_rows(latent_in_grad) * own_rows(latent_part) * own_rows(inverse_latent), axis=0
    )

    def terms(a, b, parts=None):
        return jnp.stack([matmul_tn(a[j], b[j]).astype(BF16) for j in dps])

    attn_cols = [cols(attn_in, j) for j in dps]
    expand_terms = terms([cols(latent_low, j, lat_blk) for j in dps], [expanded_grad] * n_dp)
    if (lat_blk // n_e) % 16:
        expand_terms = expand_terms.astype(F32)
    query_grad, output_grad, expand_grad, latent_grad = sum_chips(
        sizes,
        [
            terms(attn_cols, [query_raw_grad] * n_dp),
            terms([cols(hidden_low, j) for j in dps], [context_low] * n_dp),
            expand_terms,
            terms(attn_cols, [compressed_grad] * n_dp),
        ],
        [False, False, False, True],
        4,
    )
    output_grad = output_grad.T

    gains = jnp.concatenate(
        [
            unroll_columns(attn_gain_grad, blk),
            unroll_columns(ffn_gain_grad, blk),
            latent_gain_grad,
        ]
    ).reshape(-1, 128)
    gains = gains + swap(gains)
    for axis, size in (("expert", n_e), ("dp", n_dp)):
        k = 1
        while k < size:
            gains = gains + lax.ppermute(gains, axis, [(i, i ^ k) for i in range(size)])
            k *= 2
    gains = gains.reshape(-1)
    device = (dp * n_e + ex) * n_t + tn
    devices = n_dp * n_e * n_t

    def gain_part(start, length):
        size = length // devices
        return lax.dynamic_slice_in_dim(gains, start + device * size, size, 0)

    return (
        block_output,
        input_grad,
        query_grad,
        latent_grad,
        expand_grad,
        output_grad,
        sgate_grad,
        sup_grad,
        sdown_grad,
        egate_grad[None],
        eup_grad[None],
        edown_grad[None],
        gain_part(0, D),
        gain_part(2 * D, LATENT),
        gain_part(D, D),
    )


def solution(mesh):
    everyone = ("dp", "expert", "tensor")
    in_specs = (
        P(everyone, None),
        P("dp", "tensor"),
        P("dp", None),
        P("dp", "tensor"),
        P("tensor", "dp"),
        P("dp", "tensor"),
        P("dp", "tensor"),
        P("tensor", "dp"),
        P(("expert", "tensor"), "dp", None),
        P(("expert", "tensor"), "dp", None),
        P(("expert", "tensor"), None, "dp"),
        P(),
        P(),
        P(),
        P(everyone, None),
        P(everyone, None),
        P(everyone, None),
    )
    out_specs = (
        P(everyone, None),
        P(everyone, None),
        P(("dp", "expert"), "tensor"),
        P(everyone, None),
        P(("dp", "expert"), "tensor"),
        P("tensor", ("dp", "expert")),
        P(("dp", "expert"), "tensor"),
        P(("dp", "expert"), "tensor"),
        P("tensor", ("dp", "expert")),
        P(("expert", "tensor"), "dp", None),
        P(("expert", "tensor"), "dp", None),
        P(("expert", "tensor"), None, "dp"),
        P(everyone),
        P(everyone),
        P(everyone),
    )
    return jax.shard_map(body, mesh=mesh, in_specs=in_specs, out_specs=out_specs, check_vma=False)
```
